32 devices in a mesh: rep: 2 (over z, core), dp: 16 (over x, y).
Axes of the slice: x: 4, y: 4, z: 1, core: 2. Of those that a mesh axis runs over, the one named last changes fastest.
The devices are a block of a 4x4x8 slice.
Arguments:
- x: bfloat16 [32, 2048, 768], P(('rep', 'dp')), parts along dimension 0
- dy: bfloat16 [32, 2048, 768], P(('rep', 'dp')), parts along dimension 0
- wq: bfloat16 [2, 768, 768], P(None, 'dp')
- wk: bfloat16 [2, 768, 256], P(None, 'dp')
- wv: bfloat16 [2, 768, 256], P(None, 'dp')
- wo: bfloat16 [2, 768, 768], P(None, 'dp')
- w_gate: bfloat16 [2, 768, 2304], P(None, 'dp')
- w_up: bfloat16 [2, 768, 2304], P(None, 'dp')
- w_down: bfloat16 [2, 2304, 768], P(None, 'dp')
- m_wq: float32 [2, 768, 768], P(None, 'dp')
- m_wk: float32 [2, 768, 256], P(None, 'dp')
- m_wv: float32 [2, 768, 256], P(None, 'dp')
- m_wo: float32 [2, 768, 768], P(None, 'dp')
- m_w_gate: float32 [2, 768, 2304], P(None, 'dp')
- m_w_up: float32 [2, 768, 2304], P(None, 'dp')
- m_w_down: float32 [2, 2304, 768], P(None, 'dp')
- v_wq: float32 [2, 768, 768], P(None, 'dp')
- v_wk: float32 [2, 768, 256], P(None, 'dp')
- v_wv: float32 [2, 768, 256], P(None, 'dp')
- v_wo: float32 [2, 768, 768], P(None, 'dp')
- v_w_gate: float32 [2, 768, 2304], P(None, 'dp')
- v_w_up: float32 [2, 768, 2304], P(None, 'dp')
- v_w_down: float32 [2, 2304, 768], P(None, 'dp')
Outputs:
- output 1: bfloat16 [4, 768, 768], P('rep', 'dp'), parts along dimension 0
- output 2: bfloat16 [4, 768, 256], P('rep', 'dp'), parts along dimension 0
- output 3: bfloat16 [4, 768, 256], P('rep', 'dp'), parts along dimension 0
- output 4: bfloat16 [4, 768, 768], P('rep', 'dp'), parts along dimension 0
- output 5: bfloat16 [4, 768, 2304], P('rep', 'dp'), parts along dimension 0
- output 6: bfloat16 [4, 768, 2304], P('rep', 'dp'), parts along dimension 0
- output 7: bfloat16 [4, 2304, 768], P('rep', 'dp'), parts along dimension 0
- output 8: float32 [4, 768, 768], P('rep', 'dp'), parts along dimension 0
- output 9: float32 [4, 768, 256], P('rep', 'dp'), parts along dimension 0
- output 10: float32 [4, 768, 256], P('rep', 'dp'), parts along dimension 0
- output 11: float32 [4, 768, 768], P('rep', 'dp'), parts along dimension 0
- output 12: float32 [4, 768, 2304], P('rep', 'dp'), parts along dimension 0
- output 13: float32 [4, 768, 2304], P('rep', 'dp'), parts along dimension 0
- output 14: float32 [4, 2304, 768], P('rep', 'dp'), parts along dimension 0
- output 15: float32 [4, 768, 768], P('rep', 'dp'), parts along dimension 0
- output 16: float32 [4, 768, 256], P('rep', 'dp'), parts along dimension 0
- output 17: float32 [4, 768, 256], P('rep', 'dp'), parts along dimension 0
- output 18: float32 [4, 768, 768], P('rep', 'dp'), parts along dimension 0
- output 19: float32 [4, 768, 2304], P('rep', 'dp'), parts along dimension 0
- output 20: float32 [4, 768, 2304], P('rep', 'dp'), parts along dimension 0
- output 21: float32 [4, 2304, 768], P('rep', 'dp'), parts along dimension 0
There are 2 independent parts. The reference program is written for one: setup_inputs(seed, part) draws one part's arguments, and reference() takes and returns one part's arrays. A program takes and returns all parts, laid end to end along the dimension named above; an argument that names none is the same for every part.
All inputs are finite; a program needn't handle non-finite values.
Results may differ from the reference program's by a relative error of at most 0.024.
Values are sent between devices in bfloat16 or wider.
A program may use at most 768 MiB of HBM per device.

```python
import jax
import jax.numpy as jnp
from jax import lax

SEQUENCES = 16
TOKENS = 2048
D = 768
HEADS = 6
KV_HEADS = 2
HEAD = 128
FF = 2304
LAYERS = 2
THETA = 10000
NAMES = ("wq", "wk", "wv", "wo", "w_gate", "w_up", "w_down")
SHAPES = {
    "wq": (LAYERS, D, HEADS * HEAD),
    "wk": (LAYERS, D, KV_HEADS * HEAD),
    "wv": (LAYERS, D, KV_HEADS * HEAD),
    "wo": (LAYERS, HEADS * HEAD, D),
    "w_gate": (LAYERS, D, FF),
    "w_up": (LAYERS, D, FF),
    "w_down": (LAYERS, FF, D),
}


def bump(key, n, height):
    away = (jnp.arange(n, dtype=jnp.int32) - jax.random.randint(key, (), 0, n, jnp.int32)) % n
    return jnp.where(away < n // 8, height, 1.0)


def together(key, own, strength):
    shared = jax.random.normal(key, own.shape[1:], jnp.float32)
    return (own + strength * shared) * lax.rsqrt(1 + strength * strength)


def setup_inputs(seed: int = 0, part: int = 0) -> dict:
    kx, kdy, ka, kb, kz, kf, kh, kl, *keys = jax.random.split(jax.random.key(seed), 8 + 3 * len(NAMES))
    kx, kdy, ka, kb = (jax.random.fold_in(k, part) for k in (kx, kdy, ka, kb))
    kw, km, kv = (keys[i::3] for i in range(3))
    shape = (SEQUENCES, TOKENS, D)
    much_x, much_dy = jax.random.uniform(kz, (2,), jnp.float32, 0.0, 1.0)
    loud = 2.0 ** jax.random.uniform(jax.random.fold_in(kz, 1), (), jnp.float32, -1.0, 2.0)
    layers = 2.0 ** jax.random.uniform(kl, (LAYERS, 1, 1), jnp.float32, -1.0, 1.0)
    times = {"wq": 1.0, "wk": 1.0, "wv": 2.0, "wo": layers, "w_gate": 1.0, "w_up": bump(kh, FF, 4.0), "w_down": layers}
    x = together(ka, jax.random.normal(kx, shape, jnp.float32), much_x) * bump(kf, D, 4.0)
    dy = together(kb, jax.random.normal(kdy, shape, jnp.float32), much_dy)
    drawn = {"x": x.astype(jnp.bfloat16), "dy": (loud * dy * (SEQUENCES * TOKENS) ** -0.5).astype(jnp.bfloat16)}
    for key, name in zip(kw, NAMES, strict=True):
        drawn[name] = (jax.random.normal(key, SHAPES[name], jnp.float32) * SHAPES[name][1] ** -0.5 * times[name]).astype(jnp.bfloat16)
    for key, name in zip(km, NAMES, strict=True):
        drawn[f"m_{name}"] = 0.1 * jax.random.normal(key, SHAPES[name], jnp.float32)
    for key, name in zip(kv, NAMES, strict=True):
        drawn[f"v_{name}"] = jax.random.uniform(key, SHAPES[name], jnp.float32, 0.02, 0.06)
    return drawn


def matmul(a, w):
    return jnp.dot(a, w, preferred_element_type=jnp.float32).astype(jnp.bfloat16)


def normed(h):
    wide = h.astype(jnp.float32)
    scale = lax.rsqrt(jnp.mean(wide**2, -1, keepdims=True) + 1e-6)
    return (wide * scale).astype(jnp.bfloat16)


def turned(t, theta):
    half = t.shape[-1] // 2
    angle = jnp.arange(t.shape[0], dtype=jnp.float32)[:, None] * theta ** (-jnp.arange(half, dtype=jnp.float32) / half)
    cos, sin = jnp.cos(angle)[:, None], jnp.sin(angle)[:, None]
    a, b = t[..., :half].astype(jnp.float32), t[..., half:].astype(jnp.float32)
    return jnp.concatenate([a * cos - b * sin, b * cos + a * sin], -1).astype(jnp.bfloat16)


def seen_by(q, k, v):
    tokens, kv = q.shape[0], k.shape[1]
    q = q.reshape(tokens, kv, -1, q.shape[-1])
    scores = jnp.einsum("tgsd,ugd->gstu", q.astype(jnp.float32), k.astype(jnp.float32)) * q.shape[-1] ** -0.5
    place = jnp.arange(tokens)
    weights = jax.nn.softmax(jnp.where(place[:, None] >= place, scores, -jnp.inf), -1).astype(jnp.bfloat16)
    return jnp.einsum("gstu,ugd->tgsd", weights.astype(jnp.float32), v.astype(jnp.float32)).astype(jnp.bfloat16).reshape(tokens, -1)


def layer(h, w):
    a = normed(h)
    q, k = (turned(matmul(a, w[name]).reshape(h.shape[0], -1, HEAD), THETA) for name in ("wq", "wk"))
    h = h + matmul(seen_by(q, k, matmul(a, w["wv"]).reshape(h.shape[0], -1, HEAD)), w["wo"])
    b = normed(h)
    gate = jnp.dot(b, w["w_gate"], preferred_element_type=jnp.float32)
    up = jnp.dot(b, w["w_up"], preferred_element_type=jnp.float32)
    return h + matmul((jax.nn.silu(gate) * up).astype(jnp.bfloat16), w["w_down"])


def adamw(w, m, v, g):
    m = 0.9 * m + 0.1 * g
    v = 0.95 * v + 0.05 * g * g
    step = m * lax.rsqrt(v + 1e-8) + 0.1 * w
    return (w - 0.02 * step).astype(jnp.bfloat16), m, v


def clipped(gradients, sum_of_squares, count):
    factor = jnp.minimum(1.0, 0.5 * lax.rsqrt(sum_of_squares / count + 1e-30))
    return [g * factor for g in gradients]


def stack(weights, h):
    return lax.scan(lambda h, w: (layer(h, w), None), h, weights)[0]


def reference(x, dy, wq, wk, wv, wo, w_gate, w_up, w_down, m_wq, m_wk, m_wv, m_wo, m_w_gate, m_w_up, m_w_down, v_wq, v_wk, v_wv, v_wo, v_w_gate, v_w_up, v_w_down):
    weights = dict(zip(NAMES, (wq, wk, wv, wo, w_gate, w_up, w_down), strict=True))

    def take(so_far, sequence):
        h, by_y = sequence
        _, back = jax.vjp(stack, weights, h)
        by_weights, by_h = back(by_y)
        return jax.tree.map(lambda total, term: total + term.astype(jnp.float32), so_far, by_weights), by_h

    none_yet = {name: jnp.zeros(w.shape, jnp.float32) for name, w in weights.items()}
    by_weights, by_x = lax.scan(take, none_yet, (x, dy))
    gradients = [by_weights[name].astype(jnp.bfloat16).astype(jnp.float32) for name in NAMES]
    gradients = clipped(gradients, sum(jnp.sum(g * g) for g in gradients), sum(g.size for g in gradients))
    first = (m_wq, m_wk, m_wv, m_wo, m_w_gate, m_w_up, m_w_down)
    second = (v_wq, v_wk, v_wv, v_wo, v_w_gate, v_w_up, v_w_down)
    new = [adamw(weights[name].astype(jnp.float32), m, v, g) for name, m, v, g in zip(NAMES, first, second, gradients, strict=True)]
    return tuple(one[which] for which in range(3) for one in new)
```

```python
import functools

import jax
import jax.numpy as jnp
from jax import lax
from jax.experimental import pallas as pl
from jax.experimental.pallas import tpu as pltpu
from jax.sharding import PartitionSpec as P

HEAD = 128
THETA = 10000
EPS = 1e-6
NEG = -1e30
HIDDEN = 2 * NEG
LOG2E = 1.4426950408889634
VMEM = 63 * 2**20
BQ, BK = 512, 512
BQ_BACK, BK_BACK = 512, 512
TOKENS = 512
bf16, f32 = jnp.bfloat16, jnp.float32


def _dot(a, b, ca, cb):
    return lax.dot_general(a, b, (((ca,), (cb,)), ((), ())), preferred_element_type=f32)


def _params(*semantics):
    return pltpu.CompilerParams(dimension_semantics=semantics, vmem_limit_bytes=VMEM)


def _cost(flops, *arrays):
    return pl.CostEstimate(flops=int(flops), transcendentals=0, bytes_accessed=sum(a.size * a.dtype.itemsize for a in arrays))


def _tokens(width, t=TOKENS):
    return pl.BlockSpec((t, width), lambda i: (i, 0))


def _unit(pack, at):
    array, units = pack
    return pl.BlockSpec((array.shape[0], array.shape[1] // units, array.shape[2]), lambda i: (0, at, 0), pipeline_mode=pl.Buffered(1))


def _part(ref, c, parts):
    r = ref.shape[1] // parts
    return ref[:, c * r : (c + 1) * r, :].reshape(ref.shape[0] * r, ref.shape[2])


def _scaled(x):
    s = lax.rsqrt(jnp.mean(x * x, -1, keepdims=True) + EPS)
    return x * s, s


def _scaled_back(x, dn):
    n, s = _scaled(x)
    return s * (dn - n * jnp.mean(n * dn, -1, keepdims=True))


def _turn(x, cos, sin):
    return x * cos + pltpu.roll(x, HEAD // 2, 1) * sin


def _project(h_ref, w_ref, cos_ref, sin_ref, a_ref, q_ref, kv_ref):
    a = _scaled(h_ref[...].astype(f32))[0].astype(bf16)
    a_ref[...] = a
    cos, sin = cos_ref[...], sin_ref[...]
    q = _dot(a, _part(w_ref, 0, 3), 1, 0).astype(bf16).astype(f32)
    for n in range(q_ref.shape[1] // HEAD):
        at = slice(n * HEAD, (n + 1) * HEAD)
        q_ref[:, at] = _turn(q[:, at], cos, sin).astype(bf16)
    wide = kv_ref.shape[1]
    kv = _dot(a, _part(w_ref, 2, 3)[:, :wide], 1, 0).astype(bf16)
    for n in range(wide // HEAD // 2):
        at = slice(n * HEAD, (n + 1) * HEAD)
        kv_ref[:, at] = _turn(kv[:, at].astype(f32), cos, sin).astype(bf16)
    kv_ref[:, wide // 2 :] = kv[:, wide // 2 :]


def project(h, mix, at, tables, kv_wide):
    t, d = h.shape
    return pl.pallas_call(
        _project,
        grid=(t // TOKENS,),
        in_specs=[_tokens(d), _unit(mix, at), _tokens(HEAD), _tokens(HEAD)],
        out_specs=[_tokens(d), _tokens(d), _tokens(kv_wide)],
        out_shape=[jax.ShapeDtypeStruct((t, n), bf16) for n in (d, d, kv_wide)],
        compiler_params=_params("arbitrary"),
        cost_estimate=_cost(2 * t * d * (d + kv_wide), h, h, h),
        name="project",
    )(h, mix[0], *tables)


def _visible(iq, j, bq, bk):
    gap = lax.broadcasted_iota(jnp.int32, (bk, bq), 1) - lax.broadcasted_iota(jnp.int32, (bk, bq), 0)
    return gap >= j * bk - iq * bq


def _attend(q_ref, kv_ref, o_ref, lse_ref, top_s, mix_s, *, scale):
    bq = q_ref.shape[0]
    heads, kvs = q_ref.shape[1] // HEAD, kv_ref.shape[1] // HEAD // 2
    group = heads // kvs
    iq = pl.program_id(0)
    e = scale * LOG2E
    top_s[...] = jnp.full(top_s.shape, NEG, f32)
    mix_s[...] = jnp.zeros(mix_s.shape, f32)
    ones = jnp.ones((8, BK), bf16)

    def block(j, masked):
        here = pl.ds(j * BK, BK)
        keys = [kv_ref[here, i * HEAD : (i + 1) * HEAD] for i in range(kvs)]
        scores = [_dot(keys[n // group], q_ref[:, n * HEAD : (n + 1) * HEAD], 1, 1) for n in range(heads)]
        ok = _visible(iq, j, bq, BK) if masked else None
        weights, keeps = [], []
        for n, s in enumerate(scores):
            if masked:
                s = jnp.where(ok, s, HIDDEN)
            old = top_s[n : n + 1, :]
            top = jnp.maximum(old, s.max(axis=0, keepdims=True))
            top_s[n : n + 1, :] = top
            weights.append(jnp.exp2((s - top) * e).astype(bf16))
            keeps.append(jnp.exp2((old - top) * e))
        values = [jnp.concatenate([kv_ref[here, (kvs + i) * HEAD : (kvs + i + 1) * HEAD].T, ones], axis=0) for i in range(kvs)]
        for n in range(heads):
            mix_s[n] = mix_s[n] * keeps[n] + _dot(values[n // group], weights[n], 1, 0)

    whole = iq * bq // BK
    lax.fori_loop(0, whole, lambda j, _: block(j, False), None)
    for j in range(max(bq // BK, 1)):
        block(whole + j, True)
    for n in range(heads):
        total = mix_s[n, HEAD : HEAD + 1, :]
        o_ref[:, n * HEAD : (n + 1) * HEAD] = (mix_s[n, :HEAD, :] * (1 / total)).T.astype(bf16)
        lse_ref[n : n + 1, :] = (top_s[n : n + 1, :] * scale + jnp.log(total)) * LOG2E


def attend(q, kv):
    t, d = q.shape
    heads = d // HEAD
    return pl.pallas_call(
        functools.partial(_attend, scale=HEAD**-0.5),
        grid=(t // BQ,),
        in_specs=[_tokens(d, BQ), pl.BlockSpec(kv.shape, lambda i: (0, 0))],
        out_specs=[_tokens(d, BQ), pl.BlockSpec((heads, BQ), lambda i: (0, i))],
        out_shape=[jax.ShapeDtypeStruct((t, d), bf16), jax.ShapeDtypeStruct((heads, t), f32)],
        scratch_shapes=[pltpu.VMEM((heads, BQ), f32), pltpu.VMEM((heads, HEAD + 8, BQ), f32)],
        compiler_params=_params("arbitrary"),
        cost_estimate=_cost(4 * t * t * d, q, q, kv),
        name="attend",
    )(q, kv)


def _feed(h_ref, o_ref, mix_ref, wg_ref, wu_ref, wd_ref, h1_ref, b_ref, gate_ref, up_ref, act_ref, *out, last):
    h1 = (h_ref[...].astype(f32) + _dot(o_ref[...], _part(mix_ref, 1, 3), 1, 0).astype(bf16).astype(f32)).astype(bf16)
    h1_ref[...] = h1
    b_ref[...] = _scaled(h1.astype(f32))[0].astype(bf16)
    d = h1.shape[1]
    parts = gate_ref.shape[1] // d
    for c in range(parts):
        at = slice(c * d, (c + 1) * d)
        gate = _dot(b_ref[...], _part(wg_ref, c, parts), 1, 0)
        up = _dot(b_ref[...], _part(wu_ref, c, parts), 1, 0)
        gate_ref[:, at] = gate
        up_ref[:, at] = up
        act_ref[:, at] = (gate * jax.nn.sigmoid(gate) * up).astype(bf16)
    if not last:
        down = _dot(act_ref[...], wd_ref[...].reshape(parts * d, d), 1, 0).astype(bf16)
        out[0][...] = (h1_ref[...].astype(f32) + down.astype(f32)).astype(bf16)


def feed(h, o, mix, at, wide, last):
    t, d = h.shape
    ff = wide[0].shape[1] // wide[1] * wide[0].shape[0]
    outs = [(d, bf16), (d, bf16), (ff, f32), (ff, f32), (ff, bf16)] + ([] if last else [(d, bf16)])
    return pl.pallas_call(
        functools.partial(_feed, last=last),
        grid=(t // TOKENS,),
        in_specs=[_tokens(d), _tokens(d), _unit(mix, at), _unit(wide, 0), _unit(wide, 1), _unit(wide, 2)],
        out_specs=[_tokens(n) for n, _ in outs],
        out_shape=[jax.ShapeDtypeStruct((t, n), dt) for n, dt in outs],
        compiler_params=_params("arbitrary"),
        cost_estimate=_cost(2 * t * d * (d + (2 if last else 3) * ff), h, h, o),
        name="feed",
    )(h, o, mix[0], wide[0], wide[0], wide[0])


def _feed_back(dy_ref, gate_ref, up_ref, h1_ref, mix_ref, wg_ref, wu_ref, wd_ref, dg_ref, du_ref, dh1_ref, do_ref):
    dy = dy_ref[...]
    d = dy.shape[1]
    parts = gate_ref.shape[1] // d
    rows = wd_ref.shape[1] * wd_ref.shape[0]
    wd = wd_ref[...].reshape(rows, d)
    db = None
    for c in range(parts):
        at = slice(c * d, (c + 1) * d)
        dact = _dot(dy, wd[at, :], 1, 1).astype(bf16).astype(f32)
        gate = gate_ref[:, at]
        sig = jax.nn.sigmoid(gate)
        silu = gate * sig
        du = (dact * silu).astype(bf16)
        dg = (dact * up_ref[:, at] * (sig + silu * (1 - sig))).astype(bf16)
        du_ref[:, at] = du
        dg_ref[:, at] = dg
        more = _dot(dg, _part(wg_ref, c, parts), 1, 1) + _dot(du, _part(wu_ref, c, parts), 1, 1)
        db = more if db is None else db + more
    dx = _scaled_back(h1_ref[...].astype(f32), db.astype(bf16).astype(f32)).astype(bf16)
    dh1 = (dy.astype(f32) + dx.astype(f32)).astype(bf16)
    dh1_ref[...] = dh1
    do_ref[...] = _dot(dh1, _part(mix_ref, 1, 3), 1, 1).astype(bf16)


def feed_back(dy, gate, up, h1, mix, at, wide):
    t, d = dy.shape
    ff = gate.shape[1]
    step = TOKENS // 2
    outs = (ff, ff, d, d)
    return pl.pallas_call(
        _feed_back,
        grid=(t // step,),
        in_specs=[_tokens(d, step), _tokens(ff, step), _tokens(ff, step), _tokens(d, step),
                  _unit(mix, at), _unit(wide, 0), _unit(wide, 1), _unit(wide, 2)],
        out_specs=[_tokens(n, step) for n in outs],
        out_shape=[jax.ShapeDtypeStruct((t, n), bf16) for n in outs],
        compiler_params=_params("arbitrary"),
        cost_estimate=_cost(2 * t * d * (d + 3 * ff), gate, up, dy),
        name="feed_back",
    )(dy, gate, up, h1, mix[0], wide[0], wide[0], wide[0])


def _attend_back(q_ref, kv_ref, o_ref, do_ref, lse_ref, cos_ref, sin_ref, cos_all, sin_all, dq_ref, dkv_ref, dq_s, dk_s, dv_s, *, scale):
    bq = q_ref.shape[0]
    heads, kvs = q_ref.shape[1] // HEAD, kv_ref.shape[1] // HEAD // 2
    group = heads // kvs
    iq = pl.program_id(0)
    e = scale * LOG2E
    at = [slice(n * HEAD, (n + 1) * HEAD) for n in range(heads)]

    @pl.when(iq == 0)
    def _():
        dk_s[...] = jnp.zeros_like(dk_s)
        dv_s[...] = jnp.zeros_like(dv_s)

    dq_s[...] = jnp.zeros_like(dq_s)
    deltas = [(do_ref[:, a].astype(f32) * o_ref[:, a].astype(f32)).T.sum(axis=0, keepdims=True) for a in at]
    lses = [lse_ref[n : n + 1, :] for n in range(heads)]

    def block(j, masked):
        here = pl.ds(j * BK_BACK, BK_BACK)
        ok = _visible(iq, j, bq, BK_BACK) if masked else None
        for i in range(kvs):
            k = kv_ref[here, i * HEAD : (i + 1) * HEAD]
            v = kv_ref[here, (kvs + i) * HEAD : (kvs + i + 1) * HEAD]
            mine = range(i * group, (i + 1) * group)
            scores = [_dot(k, q_ref[:, at[n]], 1, 1) for n in mine]
            dps = [_dot(v, do_ref[:, at[n]], 1, 1) for n in mine]
            kt = k.T
            for n, s, dp in zip(mine, scores, dps):
                p = jnp.exp2(s * e - lses[n])
                if masked:
                    p = jnp.where(ok, p, 0.0)
                ds = (p * (dp - deltas[n])).astype(bf16)
                dv_s[i, here, :] += _dot(p.astype(bf16), do_ref[:, at[n]], 1, 0)
                dk_s[i, here, :] += _dot(ds, q_ref[:, at[n]], 1, 0)
                dq_s[n] += _dot(kt, ds, 1, 0)

    whole = iq * bq // BK_BACK
    lax.fori_loop(0, whole, lambda j, _: block(j, False), None)
    for j in range(max(bq // BK_BACK, 1)):
        block(whole + j, True)
    for n in range(heads):
        dq = (dq_s[n] * scale).T.astype(bf16).astype(f32)
        dq_ref[:, at[n]] = _turn(dq, cos_ref[...], -sin_ref[...]).astype(bf16)

    @pl.when(iq == pl.num_programs(0) - 1)
    def _():
        for i in range(kvs):
            dk = (dk_s[i] * scale).astype(bf16).astype(f32)
            dkv_ref[:, i * HEAD : (i + 1) * HEAD] = _turn(dk, cos_all[...], -sin_all[...]).astype(bf16)
            dkv_ref[:, (kvs + i) * HEAD : (kvs + i + 1) * HEAD] = dv_s[i].astype(bf16)


def attend_back(q, kv, o, do, lse, tables, after=()):
    t, d = q.shape
    heads = d // HEAD
    bq = BQ_BACK
    kvs = kv.shape[1] // HEAD // 2
    whole = pl.BlockSpec((t, HEAD), lambda i: (0, 0))
    skip = len(after)

    def kernel(*refs):
        _attend_back(*refs[:9], *refs[9 + skip :], scale=HEAD**-0.5)

    return pl.pallas_call(
        kernel,
        grid=(t // bq,),
        in_specs=[_tokens(d, bq), pl.BlockSpec(kv.shape, lambda i: (0, 0)), _tokens(d, bq), _tokens(d, bq),
                  pl.BlockSpec((heads, bq), lambda i: (0, i)), _tokens(HEAD, bq), _tokens(HEAD, bq), whole, whole]
        + [pl.BlockSpec(memory_space=pl.ANY)] * skip,
        out_specs=[_tokens(d, bq), pl.BlockSpec(kv.shape, lambda i: (0, 0))],
        out_shape=[jax.ShapeDtypeStruct((t, d), bf16), jax.ShapeDtypeStruct(kv.shape, bf16)],
        scratch_shapes=[pltpu.VMEM((heads, HEAD, bq), f32), pltpu.VMEM((kvs, t, HEAD), f32), pltpu.VMEM((kvs, t, HEAD), f32)],
        compiler_params=_params("arbitrary"),
        cost_estimate=_cost(10 * t * t * d, q, o, do, kv),
        name="attend_back",
    )(q, kv, o, do, lse, *tables, *tables, *after)


def _project_back(h_ref, dh1_ref, dq_ref, dkv_ref, mix_ref, dh_ref):
    wide = dkv_ref.shape[1]
    da = _dot(dq_ref[...], _part(mix_ref, 0, 3), 1, 1) + _dot(dkv_ref[...], _part(mix_ref, 2, 3)[:, :wide], 1, 1)
    dx = _scaled_back(h_ref[...].astype(f32), da.astype(bf16).astype(f32)).astype(bf16)
    dh_ref[...] = (dh1_ref[...].astype(f32) + dx.astype(f32)).astype(bf16)


def project_back(h, dh1, dq, dkv, mix, at):
    t, d = h.shape
    return pl.pallas_call(
        _project_back,
        grid=(t // TOKENS,),
        in_specs=[_tokens(d), _tokens(d), _tokens(d), _tokens(dkv.shape[1]), _unit(mix, at)],
        out_specs=_tokens(d),
        out_shape=jax.ShapeDtypeStruct((t, d), bf16),
        compiler_params=_params("arbitrary"),
        cost_estimate=_cost(2 * t * d * (d + dkv.shape[1]), h, dh1, dq, h),
        name="project_back",
    )(h, dh1, dq, dkv, mix[0])


def _total(n, x_ref, out_ref, got, send, recv):
    me = lax.axis_index("dp")
    rep = lax.axis_index("rep")
    peers = [lax.rem(me + k, n) for k in range(1, n)]
    barrier = pltpu.get_barrier_semaphore()
    for peer in peers:
        pl.semaphore_signal(barrier, inc=1, device_id=(rep, peer), device_id_type=pl.DeviceIdType.MESH)
    pl.semaphore_wait(barrier, n - 1)
    copies = [
        pltpu.make_async_remote_copy(src_ref=x_ref, dst_ref=got.at[k], send_sem=send.at[k], recv_sem=recv.at[k],
                                     device_id=(rep, peer), device_id_type=pl.DeviceIdType.MESH)
        for k, peer in enumerate(peers)
    ]
    for copy in copies:
        copy.start()
    for copy in copies:
        copy.wait()
    out = x_ref[...]
    for k in range(n - 1):
        out = out + got[k]
    out_ref[...] = out


def total(x, n):
    tile = jnp.full((8, 128), x, f32)
    return pl.pallas_call(
        functools.partial(_total, n),
        in_specs=[pl.BlockSpec(memory_space=pltpu.VMEM)],
        out_specs=pl.BlockSpec(memory_space=pltpu.VMEM),
        out_shape=jax.ShapeDtypeStruct((8, 128), f32),
        scratch_shapes=[pltpu.VMEM((n - 1, 8, 128), f32), pltpu.SemaphoreType.DMA((n - 1,)), pltpu.SemaphoreType.DMA((n - 1,))],
        compiler_params=pltpu.CompilerParams(collective_id=0, has_side_effects=True),
        name="total",
    )(tile)[0, 0]


def adamw(w, m, v, g):
    m = 0.9 * m + 0.1 * g
    v = 0.95 * v + 0.05 * g * g
    step = m * lax.rsqrt(v + 1e-8) + 0.1 * w
    return (w - 0.02 * step).astype(bf16), m, v


def columns(w, width):
    return [w[:, c : c + width] for c in range(0, w.shape[1], width)]


def solution(mesh):
    n = mesh.shape["dp"]

    def step(x, dy, *arrays):
        weights, m, v = (arrays[i : i + 7] for i in (0, 7, 14))
        wq, wk, wv, wo, wg, wu, wd = weights
        layers, _, d = wq.shape
        kv_wide = wk.shape[2] + wv.shape[2]

        def gathered(parts):
            return lax.all_gather(jnp.concatenate(parts, 0), "dp", axis=0, tiled=False)

        def mix_parts(l):
            kv = jnp.concatenate([wk[l], wv[l], jnp.zeros((wk.shape[1], d - kv_wide), bf16)], 1)
            return [wq[l], wo[l], kv]

        def wide_parts(l):
            return columns(wg[l], d) + columns(wu[l], d) + [wd[l]]

        packs = []
        for l in range(layers):
            if l == 0:
                mix, wide = gathered(mix_parts(l)), gathered(wide_parts(l))
                packs.append(((mix, 1), 0, (wide, 3)))
            else:
                both = gathered(wide_parts(l) + mix_parts(l))
                packs.append(((both, 4), 3, (both, 4)))

        t = x.shape[1]
        half = HEAD // 2
        angle = jnp.arange(t, dtype=f32)[:, None] * float(THETA) ** (-jnp.arange(half, dtype=f32) / half)
        cos, sin = jnp.cos(angle), jnp.sin(angle)
        tables = (jnp.concatenate([cos, cos], 1), jnp.concatenate([-sin, sin], 1))

        h, kept = x[0], []
        for l in range(layers):
            mix, at, wide = packs[l]
            last = l == layers - 1
            a, q, kv = project(h, mix, at, tables, kv_wide)
            o, lse = attend(q, kv)
            h1, b, gate, up, act, *out = feed(h, o, mix, at, wide, last)
            kept.append((h, a, q, kv, o, lse, h1, b, gate, up, act))
            h = None if last else out[0]

        def by_device(g):
            return g.reshape(n, g.shape[0] // n, g.shape[1])

        def grad(a, b):
            return _dot(a, b, 0, 0).astype(bf16)

        def packed(parts):
            return jnp.concatenate(parts, 1).reshape(-1, parts[0].shape[2])

        def scattered(pack):
            return lax.psum_scatter(pack, "dp", scatter_dimension=0, tiled=True)

        rows, low = wq.shape[1], wd.shape[1]
        mine = [None] * layers
        by_h, before = dy[0], ()
        for l in reversed(range(layers)):
            mix, at, wide = packs[l]
            h, a, q, kv, o, lse, h1, b, gate, up, act = kept[l]
            dg, du, dh1, do = feed_back(by_h, gate, up, h1, mix, at, wide)
            parts = [by_device(g) for g in columns(grad(b, dg), d) + columns(grad(b, du), d) + [grad(act, by_h), grad(o, dh1)]]
            if l == 0:
                pack, do = lax.optimization_barrier((packed(parts), do))
                r = scattered(pack)
            dq, dkv = attend_back(q, kv, o, do, lse, tables, before)
            if l > 0:
                by_h = project_back(h, dh1, dq, dkv, mix, at)
            gq, gkv = grad(a, dq), grad(a, dkv)
            if l > 0:
                gkv = jnp.concatenate([gkv, jnp.zeros((d, d - kv_wide), bf16)], 1)
                pack, by_h = lax.optimization_barrier((packed(parts + [by_device(gq), by_device(gkv)]), by_h))
                r = scattered(pack)
                before = (r,)
                qkv = [r[-2 * rows : -rows], r[-rows:]]
            else:
                terms = lax.all_to_all(jnp.concatenate([by_device(gq), by_device(gkv)], 2), "dp", 0, 0, tiled=True)
                s = jnp.sum(terms.astype(f32), 0).astype(bf16)
                qkv = [s[:, :d], s[:, d:]]
            ups = wg.shape[2] // d * rows
            pick = lambda first: jnp.concatenate([r[first + c : first + c + rows] for c in range(0, ups, rows)], 1)
            k_wide = wk.shape[2]
            mine[l] = [qkv[0], qkv[1][:, :k_wide], qkv[1][:, k_wide:kv_wide], r[2 * ups + low : 2 * ups + low + rows],
                       pick(0), pick(ups), r[2 * ups : 2 * ups + low]]
        mine = [[g.astype(f32) for g in one] for one in mine]
        squares = total(sum(jnp.sum(g * g) for one in reversed(mine) for g in one), n)
        count = n * sum(w.size for w in weights)
        factor = jnp.minimum(1.0, 0.5 * lax.rsqrt(squares / count + 1e-30))
        new = [adamw(w.astype(f32), m, v, jnp.stack([mine[l][i] for l in range(layers)]) * factor)
               for i, (w, m, v) in enumerate(zip(weights, m, v, strict=True))]
        return tuple(one[which] for which in range(3) for one in new)

    states, cut = P(("rep", "dp"), None, None), P(None, "dp", None)
    return jax.shard_map(
        step,
        mesh=mesh,
        in_specs=(states, states) + (cut,) * 21,
        out_specs=(P("rep", "dp", None),) * 21,
        check_vma=False,
    )
```

```python
import functools

import jax
import jax.numpy as jnp
from jax import lax
from jax.experimental import pallas as pl
from jax.experimental.pallas import tpu as pltpu
from jax.sharding import PartitionSpec as P

HEAD = 128
THETA = 10000
EPS = 1e-6
NEG = -1e30
HIDDEN = 2 * NEG
LOG2E = 1.4426950408889634
VMEM = 63 * 2**20
BQ, BK = 512, 512
BQ_BACK, BK_BACK = 512, 512
TOKENS = 512
bf16, f32 = jnp.bfloat16, jnp.float32


def _dot(a, b, ca, cb):
    return lax.dot_general(a, b, (((ca,), (cb,)), ((), ())), preferred_element_type=f32)


def _params(*semantics):
    return pltpu.CompilerParams(dimension_semantics=semantics, vmem_limit_bytes=VMEM)


def _cost(flops, *arrays):
    return pl.CostEstimate(flops=int(flops), transcendentals=0, bytes_accessed=sum(a.size * a.dtype.itemsize for a in arrays))


def _tokens(width, t=TOKENS):
    return pl.BlockSpec((t, width), lambda i: (i, 0))


def _unit(pack, at):
    array, units = pack
    return pl.BlockSpec((array.shape[0], array.shape[1] // units, array.shape[2]), lambda i: (0, at, 0), pipeline_mode=pl.Buffered(1))


def _part(ref, c, parts):
    r = ref.shape[1] // parts
    return ref[:, c * r : (c + 1) * r, :].reshape(ref.shape[0] * r, ref.shape[2])


def _scaled(x):
    s = lax.rsqrt(jnp.mean(x * x, -1, keepdims=True) + EPS)
    return x * s, s


def _scaled_back(x, dn):
    n, s = _scaled(x)
    return s * (dn - n * jnp.mean(n * dn, -1, keepdims=True))


def _turn(x, cos, sin):
    return x * cos + pltpu.roll(x, HEAD // 2, 1) * sin


def _project(h_ref, w_ref, cos_ref, sin_ref, a_ref, q_ref, kv_ref):
    a = _scaled(h_ref[...].astype(f32))[0].astype(bf16)
    a_ref[...] = a
    cos, sin = cos_ref[...], sin_ref[...]
    q = _dot(a, _part(w_ref, 0, 3), 1, 0).astype(bf16).astype(f32)
    for n in range(q_ref.shape[1] // HEAD):
        at = slice(n * HEAD, (n + 1) * HEAD)
        q_ref[:, at] = _turn(q[:, at], cos, sin).astype(bf16)
    wide = kv_ref.shape[1]
    kv = _dot(a, _part(w_ref, 2, 3)[:, :wide], 1, 0).astype(bf16)
    for n in range(wide // HEAD // 2):
        at = slice(n * HEAD, (n + 1) * HEAD)
        kv_ref[:, at] = _turn(kv[:, at].astype(f32), cos, sin).astype(bf16)
    kv_ref[:, wide // 2 :] = kv[:, wide // 2 :]


def project(h, mix, at, tables, kv_wide):
    t, d = h.shape
    return pl.pallas_call(
        _project,
        grid=(t // TOKENS,),
        in_specs=[_tokens(d), _unit(mix, at), _tokens(HEAD), _tokens(HEAD)],
        out_specs=[_tokens(d), _tokens(d), _tokens(kv_wide)],
        out_shape=[jax.ShapeDtypeStruct((t, n), bf16) for n in (d, d, kv_wide)],
        compiler_params=_params("arbitrary"),
        cost_estimate=_cost(2 * t * d * (d + kv_wide), h, h, h),
        name="project",
    )(h, mix[0], *tables)


def _visible(iq, j, bq, bk):
    gap = lax.broadcasted_iota(jnp.int32, (bk, bq), 1) - lax.broadcasted_iota(jnp.int32, (bk, bq), 0)
    return gap >= j * bk - iq * bq


def _attend(q_ref, kv_ref, o_ref, lse_ref, top_s, mix_s, *, scale):
    bq = q_ref.shape[0]
    heads, kvs = q_ref.shape[1] // HEAD, kv_ref.shape[1] // HEAD // 2
    group = heads // kvs
    iq = pl.program_id(0)
    e = scale * LOG2E
    top_s[...] = jnp.full(top_s.shape, NEG, f32)
    mix_s[...] = jnp.zeros(mix_s.shape, f32)
    ones = jnp.ones((8, BK), bf16)

    def block(j, masked):
        here = pl.ds(j * BK, BK)
        keys = [kv_ref[here, i * HEAD : (i + 1) * HEAD] for i in range(kvs)]
        scores = [_dot(keys[n // group], q_ref[:, n * HEAD : (n + 1) * HEAD], 1, 1) for n in range(heads)]
        ok = _visible(iq, j, bq, BK) if masked else None
        weights, keeps = [], []
        for n, s in enumerate(scores):
            if masked:
                s = jnp.where(ok, s, HIDDEN)
            old = top_s[n : n + 1, :]
            top = jnp.maximum(old, s.max(axis=0, keepdims=True))
            top_s[n : n + 1, :] = top
            weights.append(jnp.exp2((s - top) * e).astype(bf16))
            keeps.append(jnp.exp2((old - top) * e))
        values = [jnp.concatenate([kv_ref[here, (kvs + i) * HEAD : (kvs + i + 1) * HEAD].T, ones], axis=0) for i in range(kvs)]
        for n in range(heads):
            mix_s[n] = mix_s[n] * keeps[n] + _dot(values[n // group], weights[n], 1, 0)

    whole = iq * bq // BK
    lax.fori_loop(0, whole, lambda j, _: block(j, False), None)
    for j in range(max(bq // BK, 1)):
        block(whole + j, True)
    for n in range(heads):
        total = mix_s[n, HEAD : HEAD + 1, :]
        o_ref[:, n * HEAD : (n + 1) * HEAD] = (mix_s[n, :HEAD, :] * (1 / total)).T.astype(bf16)
        lse_ref[n : n + 1, :] = (top_s[n : n + 1, :] * scale + jnp.log(total)) * LOG2E


def attend(q, kv):
    t, d = q.shape
    heads = d // HEAD
    return pl.pallas_call(
        functools.partial(_attend, scale=HEAD**-0.5),
        grid=(t // BQ,),
        in_specs=[_tokens(d, BQ), pl.BlockSpec(kv.shape, lambda i: (0, 0))],
        out_specs=[_tokens(d, BQ), pl.BlockSpec((heads, BQ), lambda i: (0, i))],
        out_shape=[jax.ShapeDtypeStruct((t, d), bf16), jax.ShapeDtypeStruct((heads, t), f32)],
        scratch_shapes=[pltpu.VMEM((heads, BQ), f32), pltpu.VMEM((heads, HEAD + 8, BQ), f32)],
        compiler_params=_params("arbitrary"),
        cost_estimate=_cost(4 * t * t * d, q, q, kv),
        name="attend",
    )(q, kv)


def _feed(h_ref, o_ref, mix_ref, wg_ref, wu_ref, wd_ref, h1_ref, b_ref, gate_ref, up_ref, act_ref, *out, last):
    h1 = (h_ref[...].astype(f32) + _dot(o_ref[...], _part(mix_ref, 1, 3), 1, 0).astype(bf16).astype(f32)).astype(bf16)
    h1_ref[...] = h1
    b_ref[...] = _scaled(h1.astype(f32))[0].astype(bf16)
    d = h1.shape[1]
    parts = gate_ref.shape[1] // d
    for c in range(parts):
        at = slice(c * d, (c + 1) * d)
        gate = _dot(b_ref[...], _part(wg_ref, c, parts), 1, 0)
        up = _dot(b_ref[...], _part(wu_ref, c, parts), 1, 0)
        gate_ref[:, at] = gate
        up_ref[:, at] = up
        act_ref[:, at] = (gate * jax.nn.sigmoid(gate) * up).astype(bf16)
    if not last:
        down = _dot(act_ref[...], wd_ref[...].reshape(parts * d, d), 1, 0).astype(bf16)
        out[0][...] = (h1_ref[...].astype(f32) + down.astype(f32)).astype(bf16)


def feed(h, o, mix, at, wide, last):
    t, d = h.shape
    ff = wide[0].shape[1] // wide[1] * wide[0].shape[0]
    outs = [(d, bf16), (d, bf16), (ff, f32), (ff, f32), (ff, bf16)] + ([] if last else [(d, bf16)])
    return pl.pallas_call(
        functools.partial(_feed, last=last),
        grid=(t // TOKENS,),
        in_specs=[_tokens(d), _tokens(d), _unit(mix, at), _unit(wide, 0), _unit(wide, 1), _unit(wide, 2)],
        out_specs=[_tokens(n) for n, _ in outs],
        out_shape=[jax.ShapeDtypeStruct((t, n), dt) for n, dt in outs],
        compiler_params=_params("arbitrary"),
        cost_estimate=_cost(2 * t * d * (d + (2 if last else 3) * ff), h, h, o),
        name="feed",
    )(h, o, mix[0], wide[0], wide[0], wide[0])


def _feed_back(dy_ref, gate_ref, up_ref, h1_ref, mix_ref, wg_ref, wu_ref, wd_ref, dg_ref, du_ref, dh1_ref, do_ref):
    dy = dy_ref[...]
    d = dy.shape[1]
    parts = gate_ref.shape[1] // d
    rows = wd_ref.shape[1] * wd_ref.shape[0]
    wd = wd_ref[...].reshape(rows, d)
    db = None
    for c in range(parts):
        at = slice(c * d, (c + 1) * d)
        dact = _dot(dy, wd[at, :], 1, 1).astype(bf16).astype(f32)
        gate = gate_ref[:, at]
        sig = jax.nn.sigmoid(gate)
        silu = gate * sig
        du = (dact * silu).astype(bf16)
        dg = (dact * up_ref[:, at] * (sig + silu * (1 - sig))).astype(bf16)
        du_ref[:, at] = du
        dg_ref[:, at] = dg
        more = _dot(dg, _part(wg_ref, c, parts), 1, 1) + _dot(du, _part(wu_ref, c, parts), 1, 1)
        db = more if db is None else db + more
    dx = _scaled_back(h1_ref[...].astype(f32), db.astype(bf16).astype(f32)).astype(bf16)
    dh1 = (dy.astype(f32) + dx.astype(f32)).astype(bf16)
    dh1_ref[...] = dh1
    do_ref[...] = _dot(dh1, _part(mix_ref, 1, 3), 1, 1).astype(bf16)


def feed_back(dy, gate, up, h1, mix, at, wide):
    t, d = dy.shape
    ff = gate.shape[1]
    step = TOKENS
    outs = (ff, ff, d, d)
    return pl.pallas_call(
        _feed_back,
        grid=(t // step,),
        in_specs=[_tokens(d, step), _tokens(ff, step), _tokens(ff, step), _tokens(d, step),
                  _unit(mix, at), _unit(wide, 0), _unit(wide, 1), _unit(wide, 2)],
        out_specs=[_tokens(n, step) for n in outs],
        out_shape=[jax.ShapeDtypeStruct((t, n), bf16) for n in outs],
        compiler_params=_params("arbitrary"),
        cost_estimate=_cost(2 * t * d * (d + 3 * ff), gate, up, dy),
        name="feed_back",
    )(dy, gate, up, h1, mix[0], wide[0], wide[0], wide[0])


def _attend_back(q_ref, kv_ref, o_ref, do_ref, lse_ref, cos_ref, sin_ref, cos_all, sin_all, dq_ref, dkv_ref, dq_s, dk_s, dv_s, *, scale):
    bq = q_ref.shape[0]
    heads, kvs = q_ref.shape[1] // HEAD, kv_ref.shape[1] // HEAD // 2
    group = heads // kvs
    iq = pl.program_id(0)
    e = scale * LOG2E
    at = [slice(n * HEAD, (n + 1) * HEAD) for n in range(heads)]

    @pl.when(iq == 0)
    def _():
        dk_s[...] = jnp.zeros_like(dk_s)
        dv_s[...] = jnp.zeros_like(dv_s)

    dq_s[...] = jnp.zeros_like(dq_s)
    deltas = [(do_ref[:, a].astype(f32) * o_ref[:, a].astype(f32)).T.sum(axis=0, keepdims=True) for a in at]
    lses = [lse_ref[n : n + 1, :] for n in range(heads)]

    def block(j, masked):
        here = pl.ds(j * BK_BACK, BK_BACK)
        ok = _visible(iq, j, bq, BK_BACK) if masked else None
        for i in range(kvs):
            k = kv_ref[here, i * HEAD : (i + 1) * HEAD]
            v = kv_ref[here, (kvs + i) * HEAD : (kvs + i + 1) * HEAD]
            mine = range(i * group, (i + 1) * group)
            scores = [_dot(k, q_ref[:, at[n]], 1, 1) for n in mine]
            dps = [_dot(v, do_ref[:, at[n]], 1, 1) for n in mine]
            kt = k.T
            for n, s, dp in zip(mine, scores, dps):
                p = jnp.exp2(s * e - lses[n])
                if masked:
                    p = jnp.where(ok, p, 0.0)
                ds = (p * (dp - deltas[n])).astype(bf16)
                dv_s[i, here, :] += _dot(p.astype(bf16), do_ref[:, at[n]], 1, 0)
                dk_s[i, here, :] += _dot(ds, q_ref[:, at[n]], 1, 0)
                dq_s[n] += _dot(kt, ds, 1, 0)

    whole = iq * bq // BK_BACK
    lax.fori_loop(0, whole, lambda j, _: block(j, False), None)
    for j in range(max(bq // BK_BACK, 1)):
        block(whole + j, True)
    for n in range(heads):
        dq = (dq_s[n] * scale).T.astype(bf16).astype(f32)
        dq_ref[:, at[n]] = _turn(dq, cos_ref[...], -sin_ref[...]).astype(bf16)

    @pl.when(iq == pl.num_programs(0) - 1)
    def _():
        for i in range(kvs):
            dk = (dk_s[i] * scale).astype(bf16).astype(f32)
            dkv_ref[:, i * HEAD : (i + 1) * HEAD] = _turn(dk, cos_all[...], -sin_all[...]).astype(bf16)
            dkv_ref[:, (kvs + i) * HEAD : (kvs + i + 1) * HEAD] = dv_s[i].astype(bf16)


def attend_back(q, kv, o, do, lse, tables, after=()):
    t, d = q.shape
    heads = d // HEAD
    bq = BQ_BACK
    kvs = kv.shape[1] // HEAD // 2
    whole = pl.BlockSpec((t, HEAD), lambda i: (0, 0))
    skip = len(after)

    def kernel(*refs):
        _attend_back(*refs[:9], *refs[9 + skip :], scale=HEAD**-0.5)

    return pl.pallas_call(
        kernel,
        grid=(t // bq,),
        in_specs=[_tokens(d, bq), pl.BlockSpec(kv.shape, lambda i: (0, 0)), _tokens(d, bq), _tokens(d, bq),
                  pl.BlockSpec((heads, bq), lambda i: (0, i)), _tokens(HEAD, bq), _tokens(HEAD, bq), whole, whole]
        + [pl.BlockSpec(memory_space=pl.ANY)] * skip,
        out_specs=[_tokens(d, bq), pl.BlockSpec(kv.shape, lambda i: (0, 0))],
        out_shape=[jax.ShapeDtypeStruct((t, d), bf16), jax.ShapeDtypeStruct(kv.shape, bf16)],
        scratch_shapes=[pltpu.VMEM((heads, HEAD, bq), f32), pltpu.VMEM((kvs, t, HEAD), f32), pltpu.VMEM((kvs, t, HEAD), f32)],
        compiler_params=_params("arbitrary"),
        cost_estimate=_cost(10 * t * t * d, q, o, do, kv),
        name="attend_back",
    )(q, kv, o, do, lse, *tables, *tables, *after)


def _project_back(h_ref, dh1_ref, dq_ref, dkv_ref, mix_ref, dh_ref):
    wide = dkv_ref.shape[1]
    da = _dot(dq_ref[...], _part(mix_ref, 0, 3), 1, 1) + _dot(dkv_ref[...], _part(mix_ref, 2, 3)[:, :wide], 1, 1)
    dx = _scaled_back(h_ref[...].astype(f32), da.astype(bf16).astype(f32)).astype(bf16)
    dh_ref[...] = (dh1_ref[...].astype(f32) + dx.astype(f32)).astype(bf16)


def project_back(h, dh1, dq, dkv, mix, at):
    t, d = h.shape
    return pl.pallas_call(
        _project_back,
        grid=(t // TOKENS,),
        in_specs=[_tokens(d), _tokens(d), _tokens(d), _tokens(dkv.shape[1]), _unit(mix, at)],
        out_specs=_tokens(d),
        out_shape=jax.ShapeDtypeStruct((t, d), bf16),
        compiler_params=_params("arbitrary"),
        cost_estimate=_cost(2 * t * d * (d + dkv.shape[1]), h, dh1, dq, h),
        name="project_back",
    )(h, dh1, dq, dkv, mix[0])


def _total(n, x_ref, out_ref, got, send, recv):
    me = lax.axis_index("dp")
    rep = lax.axis_index("rep")
    peers = [lax.rem(me + k, n) for k in range(1, n)]
    barrier = pltpu.get_barrier_semaphore()
    for peer in peers:
        pl.semaphore_signal(barrier, inc=1, device_id=(rep, peer), device_id_type=pl.DeviceIdType.MESH)
    pl.semaphore_wait(barrier, n - 1)
    copies = [
        pltpu.make_async_remote_copy(src_ref=x_ref, dst_ref=got.at[k], send_sem=send.at[k], recv_sem=recv.at[k],
                                     device_id=(rep, peer), device_id_type=pl.DeviceIdType.MESH)
        for k, peer in enumerate(peers)
    ]
    for copy in copies:
        copy.start()
    for copy in copies:
        copy.wait()
    out = x_ref[...]
    for k in range(n - 1):
        out = out + got[k]
    out_ref[...] = out


def total(x, n):
    tile = jnp.full((8, 128), x, f32)
    return pl.pallas_call(
        functools.partial(_total, n),
        in_specs=[pl.BlockSpec(memory_space=pltpu.VMEM)],
        out_specs=pl.BlockSpec(memory_space=pltpu.VMEM),
        out_shape=jax.ShapeDtypeStruct((8, 128), f32),
        scratch_shapes=[pltpu.VMEM((n - 1, 8, 128), f32), pltpu.SemaphoreType.DMA((n - 1,)), pltpu.SemaphoreType.DMA((n - 1,))],
        compiler_params=pltpu.CompilerParams(collective_id=0, has_side_effects=True),
        name="total",
    )(tile)


def _swap(n, *refs):
    arrays = len(refs) // 5
    xs, outs, gots, sends, recvs = (refs[i * arrays : (i + 1) * arrays] for i in range(5))
    me = lax.axis_index("dp")
    rep = lax.axis_index("rep")
    peers = [lax.rem(me + k, n) for k in range(1, n)]
    barrier = pltpu.get_barrier_semaphore()
    for peer in peers:
        pl.semaphore_signal(barrier, inc=1, device_id=(rep, peer), device_id_type=pl.DeviceIdType.MESH)
    pl.semaphore_wait(barrier, n - 1)
    copies = [
        pltpu.make_async_remote_copy(src_ref=x.at[peer], dst_ref=got.at[k], send_sem=send.at[k], recv_sem=recv.at[k],
                                     device_id=(rep, peer), device_id_type=pl.DeviceIdType.MESH)
        for k, peer in enumerate(peers)
        for x, got, send, recv in zip(xs, gots, sends, recvs)
    ]
    for copy in copies:
        copy.start()
    for copy in copies:
        copy.wait()
    for x, out, got in zip(xs, outs, gots):
        total = x[me].astype(f32)
        for k in range(n - 1):
            total = total + got[k].astype(f32)
        out[...] = total.astype(bf16)


def swap(xs, n):
    spec = pl.BlockSpec(memory_space=pltpu.VMEM)
    return pl.pallas_call(
        functools.partial(_swap, n),
        in_specs=[spec] * len(xs),
        out_specs=[spec] * len(xs),
        out_shape=[jax.ShapeDtypeStruct(x.shape[1:], x.dtype) for x in xs],
        scratch_shapes=[pltpu.VMEM((n - 1, *x.shape[1:]), x.dtype) for x in xs] + [pltpu.SemaphoreType.DMA((n - 1,))] * (2 * len(xs)),
        compiler_params=pltpu.CompilerParams(collective_id=1, has_side_effects=True),
        name="swap",
    )(*xs)


def _update(squares_ref, *refs, count, layers, places):
    grads, refs = refs[: layers + 2], refs[layers + 2 :]
    w, m, v, new_w, new_m, new_v = (refs[i * 7 : (i + 1) * 7] for i in range(6))
    factor = jnp.minimum(1.0, 0.5 * lax.rsqrt(squares_ref[0:1, 0:1] / count + 1e-30))
    for l in range(layers):
        for i in range(7):
            blocks = places[l][i]
            rows, width = w[i].shape[1], w[i].shape[2] // len(blocks)
            for c, (source, row, column) in enumerate(blocks):
                at = slice(c * width, (c + 1) * width)
                g = grads[source][row : row + rows, column : column + width].astype(f32) * factor
                one = 0.9 * m[i][l, :, at] + 0.1 * g
                two = 0.95 * v[i][l, :, at] + 0.05 * g * g
                step = one * lax.rsqrt(two + 1e-8) + 0.1 * w[i][l, :, at].astype(f32)
                new_w[i][l, :, at] = (w[i][l, :, at].astype(f32) - 0.02 * step).astype(bf16)
                new_m[i][l, :, at] = one
                new_v[i][l, :, at] = two


def update(squares, grads, weights, m, v, count, places):
    spec = pl.BlockSpec(memory_space=pltpu.VMEM)
    given = [squares, *grads, *weights, *m, *v]
    return pl.pallas_call(
        functools.partial(_update, count=count, layers=weights[0].shape[0], places=places),
        in_specs=[spec] * len(given),
        out_specs=[spec] * 21,
        out_shape=[jax.ShapeDtypeStruct(x.shape, x.dtype) for x in (*weights, *m, *v)],
        compiler_params=pltpu.CompilerParams(vmem_limit_bytes=VMEM),
        cost_estimate=_cost(20 * sum(w.size for w in weights), *given, *given),
        name="update",
    )(*given)


def columns(w, width):
    return [w[:, c : c + width] for c in range(0, w.shape[1], width)]


def solution(mesh):
    n = mesh.shape["dp"]

    def step(x, dy, *arrays):
        weights, m, v = (arrays[i : i + 7] for i in (0, 7, 14))
        wq, wk, wv, wo, wg, wu, wd = weights
        layers, _, d = wq.shape
        kv_wide = wk.shape[2] + wv.shape[2]

        def gathered(parts):
            return lax.all_gather(jnp.concatenate(parts, 0), "dp", axis=0, tiled=False)

        def mix_parts(l):
            kv = jnp.concatenate([wk[l], wv[l], jnp.zeros((wk.shape[1], d - kv_wide), bf16)], 1)
            return [wq[l], wo[l], kv]

        def wide_parts(l):
            return columns(wg[l], d) + columns(wu[l], d) + [wd[l]]

        packs = []
        mix, at = (gathered(mix_parts(0)), 1), 0
        for l in range(layers):
            last = l == layers - 1
            units = 3 if last else 4
            wide = (gathered(wide_parts(l) + ([] if last else mix_parts(l + 1))), units)
            packs.append((mix, at, wide))
            mix, at = wide, 3

        t = x.shape[1]
        half = HEAD // 2
        angle = jnp.arange(t, dtype=f32)[:, None] * float(THETA) ** (-jnp.arange(half, dtype=f32) / half)
        cos, sin = jnp.cos(angle), jnp.sin(angle)
        tables = (jnp.concatenate([cos, cos], 1), jnp.concatenate([-sin, sin], 1))

        h, kept = x[0], []
        for l in range(layers):
            mix, at, wide = packs[l]
            last = l == layers - 1
            a, q, kv = project(h, mix, at, tables, kv_wide)
            o, lse = attend(q, kv)
            h1, b, gate, up, act, *out = feed(h, o, mix, at, wide, last)
            kept.append((h, a, q, kv, o, lse, h1, b, gate, up, act))
            h = None if last else out[0]

        def by_device(g):
            return g.reshape(n, g.shape[0] // n, g.shape[1])

        def grad(a, b):
            return _dot(a, b, 0, 0).astype(bf16)

        def packed(parts):
            return jnp.concatenate(parts, 1).reshape(-1, parts[0].shape[2])

        def scattered(pack):
            return lax.psum_scatter(pack, "dp", scatter_dimension=0, tiled=True)

        rows, low = wq.shape[1], wd.shape[1]
        grads = [None] * layers
        by_h, before = dy[0], ()
        for l in reversed(range(layers)):
            mix, at, wide = packs[l]
            h, a, q, kv, o, lse, h1, b, gate, up, act = kept[l]
            dg, du, dh1, do = feed_back(by_h, gate, up, h1, mix, at, wide)
            parts = [by_device(g) for g in columns(grad(b, dg), d) + columns(grad(b, du), d) + [grad(act, by_h), grad(o, dh1)]]
            if l == 0:
                pack, do, *before = lax.optimization_barrier((packed(parts), do, *before))
                r = scattered(pack)
            dq, dkv = attend_back(q, kv, o, do, lse, tables, before)
            if l > 0:
                by_h = project_back(h, dh1, dq, dkv, mix, at)
            gq, gkv = grad(a, dq), grad(a, dkv)
            if l > 0:
                gkv = jnp.concatenate([gkv, jnp.zeros((d, d - kv_wide), bf16)], 1)
                pack, by_h = lax.optimization_barrier((packed(parts + [by_device(gq), by_device(gkv)]), by_h))
                r = scattered(pack)
                before = (r,)
                grads[l] = r
            else:
                grads[l] = r
                mine = swap([by_device(gq), by_device(gkv)], n)
        squares = total(sum(jnp.sum(g.astype(f32) ** 2) for g in (*reversed(grads), *mine)), n)
        places = []
        k_wide, ups = wk.shape[2], wg.shape[2] // d
        for l in range(layers):
            base = 2 * ups * rows + low
            q, kv = ((layers, 0), (layers + 1, 0)) if l == 0 else ((l, base + rows), (l, base + 2 * rows))
            places.append((((*q, 0),), ((*kv, 0),), ((*kv, k_wide),), ((l, base, 0),),
                           tuple((l, c * rows, 0) for c in range(ups)), tuple((l, (ups + c) * rows, 0) for c in range(ups)),
                           ((l, 2 * ups * rows, 0),)))
        return tuple(update(squares, [*grads, *mine], weights, m, v, n * sum(w.size for w in weights), places))

    states, cut = P(("rep", "dp"), None, None), P(None, "dp", None)
    return jax.shard_map(
        step,
        mesh=mesh,
        in_specs=(states, states) + (cut,) * 21,
        out_specs=(P("rep", "dp", None),) * 21,
        check_vma=False,
    )
```
